32 devices in a mesh: band: 4 (over z), px: 4 (over x, core), py: 2 (over y).
Axes of the slice: x: 2, y: 2, z: 4, core: 2. Of those that a mesh axis runs over, the one named last changes fastest.
Arguments:
- orbitals: bfloat16 [4, 1024, 384], P('band', ('px', 'py')), may hold values from -0.01171875 to 0.01171875
- occupations: float32 [4], P('band'), may hold values from 0.2 to 2
- stick_map: int32 [2, 1024], P(None, 'px'), may hold values from 0 to 191, as said below
- core_density: float32 [192, 192, 192], P('py', 'px'), may hold values from 0.05 to 0.5
Outputs:
- potential: float32 [192, 192, 192], P('py', 'px')
- gradient: float32 [3, 192, 192, 192], P(None, 'py', 'px')
The draws below stay inside these ranges and needn't reach their ends.
Inputs may be any that keep to these rules, and one draw needn't show every extreme that they name: `stick_map`: columns i * 128 * 2 to (i + 1) * 128 * 2 - 1 have x index from i * 48 to (i + 1) * 48 - 1; no two columns share a grid position.
All inputs are finite; a program needn't handle non-finite values.
Results may differ from the reference program's by a relative error of at most 0.0054.
Values may be sent and summed in bfloat16 or wider, within the bound.
A program may use at most 128 MiB of HBM per device.

```python
import math
import jax
import jax.numpy as jnp
from jax import lax

NG = 192
STK_DEV = 128
BANDS = 4
STICKS = 1024
N_PX = 4
N_PY = 2


def draw_stick_map(key, part):
    per_block = STK_DEV * N_PY
    xblock = NG // N_PX
    block_keys = jax.random.split(key, N_PX)

    def pick_block(one_key):
        return jax.random.permutation(one_key, xblock * NG)[:per_block]
    chosen = jax.vmap(pick_block)(block_keys)
    offsets = jnp.arange(N_PX, dtype=jnp.int32)[:, None] * xblock
    x_pos = offsets + chosen // NG
    y_pos = chosen % NG
    return jnp.stack([x_pos.reshape(-1), y_pos.reshape(-1)]).astype(jnp.int32)


def level_of(stream_key, shape, pieces, least, largest):
    def one(position, parts):
        heights = jax.random.uniform(jax.random.fold_in(jax.random.fold_in(stream_key, 6), position), (parts,), jnp.float32, least / len(pieces), largest / len(pieces))
        return jnp.repeat(jnp.exp(heights), shape[position] // parts).reshape((-1,) + (1,) * (len(shape) - position - 1))

    loudness = one(*pieces[0])
    for cut in pieces[1:]:
        loudness = loudness * one(*cut)
    return loudness


def scatter_about(own_key, dims, spread, limit, cuts=(), kind=jnp.bfloat16):
    entries = spread * jax.random.normal(own_key, dims, jnp.float32)
    if cuts:
        entries = entries * level_of(own_key, dims, cuts, -0.22, 0.18)
    return jnp.clip(entries, -limit, limit).astype(kind)


def setup_inputs(seed: int = 0) -> dict:
    seeds = jax.random.split(jax.random.key(seed), 5)
    orbitals = scatter_about(seeds[0], (BANDS, STICKS, 2 * NG), ((2 * STICKS * NG * BANDS) ** -0.5), 0.01171875, ((0, 4), (1, 8)))
    occupations = jnp.clip(0.2 + 1.8 * jax.random.uniform(seeds[1], (BANDS,), jnp.float32) ** level_of(seeds[1], (BANDS,), ((0, 4),), -0.2, 0.2), 0.2, 2.0)
    stick_map = draw_stick_map(jax.random.fold_in(seeds[4], 71), 0)
    core_density = jnp.clip(jnp.exp(math.log(0.5) - 2.3025851 * jax.random.uniform(seeds[3], (NG, NG, NG), jnp.float32) ** level_of(seeds[3], (NG, NG, NG), ((0, 2), (1, 4)), -0.2, 0.2)), 0.05, 0.5)
    return dict(orbitals=orbitals, occupations=occupations, stick_map=stick_map, core_density=core_density)


SPACING = 0.25
PBE_KAPPA = 0.804
PBE_MU = 0.2195
SLATER_COEF = 0.75 * (3.0 / math.pi) ** (1.0 / 3.0)
REDUCED_SCALE = 4.0 * (3.0 * math.pi ** 2) ** (2.0 / 3.0)


def rounded(values):
    return lax.optimization_barrier(values.astype(jnp.bfloat16)).astype(jnp.float32)


def exchange_part(density, hartree, grad_x, grad_y, grad_z):
    cube_root = jnp.cbrt(density)
    four_thirds = density * cube_root
    grad_square = grad_x * grad_x + grad_y * grad_y + grad_z * grad_z
    reduced = grad_square / (REDUCED_SCALE * four_thirds * four_thirds)
    denominator = 1.0 + PBE_MU * reduced / PBE_KAPPA
    enhance = 1.0 + PBE_KAPPA - PBE_KAPPA / denominator
    enhance_slope = PBE_MU / (denominator * denominator)
    return hartree - SLATER_COEF * cube_root * ((4.0 / 3.0) * enhance - (8.0 / 3.0) * reduced * enhance_slope)


def reference(orbitals, occupations, stick_map, core_density):
    points = orbitals.shape[2] // 2
    x_cols = stick_map[0]
    y_cols = stick_map[1]

    def add_band(summed, inputs):
        coeffs, weight = inputs
        real_in = coeffs[:, :points].astype(jnp.float32)
        imag_in = coeffs[:, points:].astype(jnp.float32)
        along_z = jnp.fft.ifft(real_in + 1j * imag_in, axis=1) * points
        plane_real = jnp.zeros((points, points, points), jnp.float32).at[:, y_cols, x_cols].set(rounded(along_z.real).T)
        plane_imag = jnp.zeros((points, points, points), jnp.float32).at[:, y_cols, x_cols].set(rounded(along_z.imag).T)
        along_y = jnp.fft.ifft(plane_real + 1j * plane_imag, axis=1) * points
        along_x = jnp.fft.ifft(rounded(along_y.real) + 1j * rounded(along_y.imag), axis=2) * points
        return summed + weight * (along_x.real * along_x.real + along_x.imag * along_x.imag), None

    valence = lax.scan(add_band, jnp.zeros((points, points, points), jnp.float32), (orbitals, occupations))[0]
    density = valence + core_density
    rho_hat = jnp.fft.fftn(density)
    every_index = jnp.arange(points)
    q_full = jnp.where(every_index <= points // 2, every_index, every_index - points).astype(jnp.float32)
    g_full = jnp.where(every_index == points // 2, 0.0, q_full).astype(jnp.float32)
    wave_unit = 2.0 * math.pi / (points * SPACING)
    squared = wave_unit ** 2 * (q_full[:, None, None] ** 2 + q_full[None, :, None] ** 2 + q_full[None, None, :] ** 2)
    hartree_factor = jnp.where(squared > 0, 4.0 * math.pi / jnp.where(squared > 0, squared, 1.0), 0.0)
    hartree = jnp.fft.ifftn(hartree_factor * rho_hat).real
    grad_x = jnp.fft.ifftn(1j * wave_unit * g_full[None, None, :] * rho_hat).real
    grad_y = jnp.fft.ifftn(1j * wave_unit * g_full[None, :, None] * rho_hat).real
    grad_z = jnp.fft.ifftn(1j * wave_unit * g_full[:, None, None] * rho_hat).real
    potential = exchange_part(density, hartree, grad_x, grad_y, grad_z)
    return potential, jnp.stack([grad_x, grad_y, grad_z])
```

```python
import math

import jax
import jax.numpy as jnp
import numpy as np
from jax import lax
from jax.experimental.layout import Layout, with_layout_constraint
from jax.sharding import PartitionSpec as P

SPACING = 0.25
PBE_KAPPA = 0.804
PBE_MU = 0.2195
SLATER_COEF = 0.75 * (3.0 / math.pi) ** (1.0 / 3.0)
REDUCED_SCALE = 4.0 * (3.0 * math.pi**2) ** (2.0 / 3.0)
BF = jnp.bfloat16
F32 = jnp.float32
HIGH = lax.Precision.HIGH


def inverse_table(points):
    k = np.arange(points)
    angles = 2.0 * np.pi / points * (k[:, None] * k[None, :] % points)
    cosine, sine = np.cos(angles), np.sin(angles)
    return np.stack([np.stack([cosine, sine], 1), np.stack([-sine, cosine], 1)], 0)


def two_halves(table):
    high = table.astype(np.float32).astype(BF)
    low = (table - high.astype(np.float64)).astype(np.float32).astype(BF)
    return high, low


def dot2(spec, data, table):
    high, low = table
    first = jnp.einsum(spec, data, high, preferred_element_type=F32)
    return first + jnp.einsum(spec, data, low, preferred_element_type=F32)


def real_basis(points):
    pos = np.arange(points)
    freq = np.concatenate([np.arange(points // 2 + 1), np.arange(1, points // 2)])
    angle = 2.0 * np.pi / points * (pos[:, None] * freq[None, :] % points)
    basis = np.where(np.arange(points)[None, :] <= points // 2, np.cos(angle), np.sin(angle))
    scale = np.where((freq == 0) | (freq == points // 2), 1.0 / points, 2.0 / points)
    return basis * np.sqrt(scale), freq


def derivative_matrix(points):
    pos = np.arange(points)
    freq = np.arange(1, points // 2)
    unit = 2.0 * np.pi / (points * SPACING)
    lag = (pos[None, :] - pos[:, None]) % points
    values = np.zeros(points)
    for d in range(points):
        values[d] = np.sum(-2.0 * unit * freq * np.sin(2.0 * np.pi * (freq * d % points) / points)) / points
    return values[lag]


def exchange_part(density, hartree, grad_x, grad_y, grad_z):
    cube_root = jnp.cbrt(density)
    four_thirds = density * cube_root
    grad_square = grad_x * grad_x + grad_y * grad_y + grad_z * grad_z
    reduced = grad_square / (REDUCED_SCALE * four_thirds * four_thirds)
    denominator = 1.0 + PBE_MU * reduced / PBE_KAPPA
    enhance = 1.0 + PBE_KAPPA - PBE_KAPPA / denominator
    enhance_slope = PBE_MU / (denominator * denominator)
    return hartree - SLATER_COEF * cube_root * (
        4.0 / 3.0 * enhance - 8.0 / 3.0 * reduced * enhance_slope
    )


def partial_density(orbitals, occupations, stick_map, px_index):
    bands_here, columns_here, doubled = orbitals.shape
    points = doubled // 2
    rows_px = lax.axis_size("px")
    rows_py = lax.axis_size("py")
    xblock = points // rows_px
    zblock = points // rows_py
    inverse = inverse_table(points)
    z_table = two_halves(
        inverse.reshape(2, points, 2, rows_py, zblock).transpose(0, 1, 3, 2, 4).reshape(doubled, doubled)
    )
    columns = dot2("bsk,kw->bsw", orbitals, z_table).astype(BF)
    columns = lax.all_to_all(columns, "py", split_axis=2, concat_axis=1, tiled=True)
    sticks = columns.shape[1]
    columns = columns.reshape(bands_here, sticks, 2, zblock)
    y_hot = (stick_map[1][:, None] == jnp.arange(points, dtype=jnp.int32)[None, :]).astype(BF)
    x_local = stick_map[0] - px_index * xblock
    x_hot = x_local[:, None] == jnp.arange(xblock, dtype=jnp.int32)[None, :]
    by_y = inverse.reshape(2, points, 2, rows_px, xblock).transpose(1, 0, 3, 4, 2)
    picked = [
        jnp.einsum("sy,yipwo->sipwo", y_hot, half, preferred_element_type=F32).astype(BF)
        for half in two_halves(by_y)
    ]
    x_table = two_halves(inverse.reshape(2, rows_px, xblock, 2, points).transpose(1, 0, 2, 3, 4))
    total = None
    for band in range(bands_here):
        spread = jnp.where(x_hot[:, None, :, None], columns[band][:, :, None, :], jnp.zeros((), BF))
        plane = jnp.einsum("sipwo,sixz->pwoxz", picked[0], spread, preferred_element_type=F32)
        plane = plane + jnp.einsum("sipwo,sixz->pwoxz", picked[1], spread, preferred_element_type=F32)
        plane = plane.astype(BF)
        plane = lax.all_to_all(plane, "px", split_axis=0, concat_axis=0, tiled=True)
        values = dot2("pwoxz,poxtk->wztk", plane, x_table)
        weighted = occupations[band] * (values[:, :, 0] * values[:, :, 0] + values[:, :, 1] * values[:, :, 1])
        total = weighted if total is None else total + weighted
    return total


def gathered(field):
    field = with_layout_constraint(field.astype(BF), Layout((0, 1, 2)))
    return lax.all_gather(field, "band", axis=0, tiled=True)


def body(orbitals, occupations, stick_map, core_density):
    points = orbitals.shape[2] // 2
    rows_px = lax.axis_size("px")
    rows_py = lax.axis_size("py")
    groups = lax.axis_size("band")
    px_index = lax.axis_index("px")
    py_index = lax.axis_index("py")
    band_index = lax.axis_index("band")
    yblock = points // rows_px
    xblock = points // rows_px
    zblock = points // rows_py
    zshare = zblock // groups
    pieces = groups * rows_py
    kyblock = points // pieces

    density = partial_density(orbitals, occupations, stick_map, px_index)
    shares = density.astype(BF).reshape(yblock, groups, zshare, points).transpose(1, 0, 2, 3)
    shares = lax.all_to_all(shares, "band", split_axis=0, concat_axis=0, tiled=True)
    core = lax.dynamic_slice_in_dim(core_density, band_index * zshare, zshare, 0)
    rho = shares.astype(F32).sum(0) + core.transpose(1, 0, 2)

    basis, freq = real_basis(points)
    derive = derivative_matrix(points).astype(np.float32)
    basis32 = basis.astype(np.float32)
    data = jnp.einsum("yzx,xpk->pyzk", rho, basis32.reshape(points, rows_px, xblock), precision=HIGH)
    data = lax.all_to_all(data, "px", split_axis=0, concat_axis=0, tiled=True)
    data = data.reshape(points, zshare, xblock)
    high_basis, low_basis = two_halves(basis)
    x_basis = (high_basis.reshape(points, rows_px, xblock), low_basis.reshape(points, rows_px, xblock))
    grad_x = jnp.einsum("yzx,xw->zyw", rho, derive, precision=HIGH)
    every_x = gathered(grad_x)
    lines_y = jnp.einsum("yzk,yw->wzk", data, derive, precision=HIGH).astype(BF)
    lines_y = lines_y.reshape(rows_px, yblock, zshare, xblock)
    lines_y = lax.all_to_all(lines_y, "px", split_axis=0, concat_axis=0, tiled=True)
    grad_y = dot2("pyzk,xpk->zyx", lines_y, x_basis)
    grad_y_sent = grad_y.astype(BF)
    modes = jnp.einsum("yzk,yj->jzk", data, basis32, precision=HIGH)
    modes = modes.reshape(pieces, kyblock, zshare, xblock)
    modes = lax.all_to_all(modes, ("band", "py"), split_axis=0, concat_axis=0, tiled=True)
    source = np.arange(points)
    device, within = source // zshare, source % zshare
    z_order = device % rows_py * zblock + device // rows_py * zshare + within
    z_basis = basis32[z_order].reshape(pieces, zshare, points)
    z_derive = derive[z_order][:, z_order].reshape(pieces, zshare, pieces, zshare)
    spectrum = jnp.einsum("djzk,dzm->mjk", modes, z_basis, precision=HIGH)
    unit = 2.0 * math.pi / (points * SPACING)
    all_q = jnp.asarray((freq * freq).astype(np.float32))
    q_col = lax.dynamic_slice_in_dim(all_q, (band_index * rows_py + py_index) * kyblock, kyblock)
    q_row = lax.dynamic_slice_in_dim(all_q, px_index * xblock, xblock)
    squared = unit**2 * (all_q[:, None, None] + q_col[None, :, None] + q_row[None, None, :])
    factor = jnp.where(squared > 0, 4.0 * math.pi / jnp.where(squared > 0, squared, 1.0), 0.0)
    spectrum = spectrum * factor
    back = jnp.stack(
        [
            jnp.einsum("mjk,dzm->djzk", spectrum, z_basis, precision=HIGH).astype(BF),
            jnp.einsum("ejwk,ewdz->djzk", modes, z_derive, precision=HIGH).astype(BF),
        ],
        1,
    )
    back, every_y = lax.optimization_barrier((back, grad_y_sent))
    every_y = gathered(every_y)
    back = lax.all_to_all(back, ("band", "py"), split_axis=0, concat_axis=0, tiled=True)
    y_basis = (high_basis.reshape(points, pieces, kyblock), low_basis.reshape(points, pieces, kyblock))
    lines = dot2("dfjzk,ydj->fyzk", back, y_basis)
    lines = lines.astype(BF).reshape(2, rows_px, yblock, zshare, xblock)
    lines = lax.all_to_all(lines, "px", split_axis=1, concat_axis=1, tiled=True)
    fields = dot2("fpyzk,xpk->fzyx", lines, x_basis)
    every_z = gathered(fields[1])
    potential = exchange_part(rho.transpose(1, 0, 2), fields[0], grad_x, grad_y, fields[1])
    every_potential = gathered(potential)
    gradient = jnp.stack([every_x.astype(F32), every_y.astype(F32), every_z.astype(F32)])
    return (every_potential.astype(F32), gradient)


def solution(mesh):
    return jax.shard_map(
        body,
        mesh=mesh,
        in_specs=(P("band", ("px", "py"), None), P("band"), P(None, "px"), P("py", "px", None)),
        out_specs=(P("py", "px", None), P(None, "py", "px", None)),
        check_vma=False,
    )
```

```python
import math

import jax
import jax.numpy as jnp
import numpy as np
from jax import lax
from jax.experimental.layout import Layout, with_layout_constraint
from jax.sharding import PartitionSpec as P

SPACING = 0.25
PBE_KAPPA = 0.804
PBE_MU = 0.2195
SLATER_COEF = 0.75 * (3.0 / math.pi) ** (1.0 / 3.0)
REDUCED_SCALE = 4.0 * (3.0 * math.pi**2) ** (2.0 / 3.0)
BF = jnp.bfloat16
F32 = jnp.float32
HIGH = lax.Precision.HIGH


def inverse_table(points):
    k = np.arange(points)
    angles = 2.0 * np.pi / points * (k[:, None] * k[None, :] % points)
    cosine, sine = np.cos(angles), np.sin(angles)
    return np.stack([np.stack([cosine, sine], 1), np.stack([-sine, cosine], 1)], 0)


def two_halves(table):
    high = table.astype(np.float32).astype(BF)
    low = (table - high.astype(np.float64)).astype(np.float32).astype(BF)
    return high, low


def dot2(spec, data, table):
    high, low = table
    first = jnp.einsum(spec, data, high, preferred_element_type=F32)
    return first + jnp.einsum(spec, data, low, preferred_element_type=F32)


def real_basis(points):
    pos = np.arange(points)
    freq = np.concatenate([np.arange(points // 2 + 1), np.arange(1, points // 2)])
    angle = 2.0 * np.pi / points * (pos[:, None] * freq[None, :] % points)
    basis = np.where(np.arange(points)[None, :] <= points // 2, np.cos(angle), np.sin(angle))
    scale = np.where((freq == 0) | (freq == points // 2), 1.0 / points, 2.0 / points)
    return basis * np.sqrt(scale), freq


def derivative_matrix(points):
    pos = np.arange(points)
    freq = np.arange(1, points // 2)
    unit = 2.0 * np.pi / (points * SPACING)
    lag = (pos[None, :] - pos[:, None]) % points
    values = np.zeros(points)
    for d in range(points):
        values[d] = np.sum(-2.0 * unit * freq * np.sin(2.0 * np.pi * (freq * d % points) / points)) / points
    return values[lag]


def exchange_part(density, hartree, grad_x, grad_y, grad_z):
    cube_root = jnp.cbrt(density)
    four_thirds = density * cube_root
    grad_square = grad_x * grad_x + grad_y * grad_y + grad_z * grad_z
    reduced = grad_square / (REDUCED_SCALE * four_thirds * four_thirds)
    denominator = 1.0 + PBE_MU * reduced / PBE_KAPPA
    enhance = 1.0 + PBE_KAPPA - PBE_KAPPA / denominator
    enhance_slope = PBE_MU / (denominator * denominator)
    return hartree - SLATER_COEF * cube_root * (
        4.0 / 3.0 * enhance - 8.0 / 3.0 * reduced * enhance_slope
    )


def partial_density(orbitals, occupations, stick_map, px_index):
    bands_here, columns_here, doubled = orbitals.shape
    points = doubled // 2
    rows_px = lax.axis_size("px")
    rows_py = lax.axis_size("py")
    xblock = points // rows_px
    zblock = points // rows_py
    inverse = inverse_table(points)
    z_table = two_halves(
        inverse.reshape(2, points, 2, rows_py, zblock).transpose(0, 1, 3, 2, 4).reshape(doubled, doubled)
    )
    columns = dot2("bsk,kw->bsw", orbitals, z_table).astype(BF)
    columns = lax.all_to_all(columns, "py", split_axis=2, concat_axis=1, tiled=True)
    sticks = columns.shape[1]
    columns = columns.reshape(bands_here, sticks, 2, zblock)
    y_hot = (stick_map[1][:, None] == jnp.arange(points, dtype=jnp.int32)[None, :]).astype(BF)
    x_local = stick_map[0] - px_index * xblock
    x_hot = x_local[:, None] == jnp.arange(xblock, dtype=jnp.int32)[None, :]
    by_y = inverse.reshape(2, points, 2, rows_px, xblock).transpose(1, 0, 3, 4, 2)
    picked = [
        jnp.einsum("sy,yipwo->sipwo", y_hot, half, preferred_element_type=F32).astype(BF)
        for half in two_halves(by_y)
    ]
    x_table = two_halves(inverse.reshape(2, rows_px, xblock, 2, points).transpose(1, 0, 2, 3, 4))
    total = None
    for band in range(bands_here):
        spread = jnp.where(x_hot[:, None, :, None], columns[band][:, :, None, :], jnp.zeros((), BF))
        plane = jnp.einsum("sipwo,sixz->pwoxz", picked[0], spread, preferred_element_type=F32)
        plane = plane + jnp.einsum("sipwo,sixz->pwoxz", picked[1], spread, preferred_element_type=F32)
        plane = plane.astype(BF)
        plane = lax.all_to_all(plane, "px", split_axis=0, concat_axis=0, tiled=True)
        values = dot2("pwoxz,poxtk->wztk", plane, x_table)
        weighted = occupations[band] * (values[:, :, 0] * values[:, :, 0] + values[:, :, 1] * values[:, :, 1])
        total = weighted if total is None else total + weighted
    return total


def gathered(field):
    field = with_layout_constraint(field.astype(BF), Layout((0, 1, 2)))
    return lax.all_gather(field, "band", axis=0, tiled=True)


def body(orbitals, occupations, stick_map, core_density):
    points = orbitals.shape[2] // 2
    rows_px = lax.axis_size("px")
    rows_py = lax.axis_size("py")
    groups = lax.axis_size("band")
    px_index = lax.axis_index("px")
    py_index = lax.axis_index("py")
    band_index = lax.axis_index("band")
    yblock = points // rows_px
    xblock = points // rows_px
    zblock = points // rows_py
    zshare = zblock // groups
    pieces = groups * rows_py
    kyblock = points // pieces

    density = partial_density(orbitals, occupations, stick_map, px_index)
    shares = density.astype(BF).reshape(yblock, groups, zshare, points).transpose(1, 0, 2, 3)
    shares = lax.all_to_all(shares, "band", split_axis=0, concat_axis=0, tiled=True)
    core = lax.dynamic_slice_in_dim(core_density, band_index * zshare, zshare, 0)
    rho = shares.astype(F32).sum(0) + core.transpose(1, 0, 2)

    basis, freq = real_basis(points)
    derive = derivative_matrix(points).astype(np.float32)
    basis32 = basis.astype(np.float32)
    data = jnp.einsum("yzx,xpk->pyzk", rho, basis32.reshape(points, rows_px, xblock), precision=HIGH)
    grad_x = jnp.einsum("yzx,xw->zyw", rho, derive, precision=HIGH)
    data, grad_x_sent = lax.optimization_barrier((data, grad_x.astype(BF)))
    every_x = gathered(grad_x_sent)
    data = lax.all_to_all(data, "px", split_axis=0, concat_axis=0, tiled=True)
    data = data.reshape(points, zshare, xblock)
    high_basis, low_basis = two_halves(basis)
    x_basis = (high_basis.reshape(points, rows_px, xblock), low_basis.reshape(points, rows_px, xblock))
    lines_y = jnp.einsum("yzk,yw->wzk", data, derive, precision=HIGH).astype(BF)
    lines_y = lines_y.reshape(rows_px, yblock, zshare, xblock)
    lines_y = lax.all_to_all(lines_y, "px", split_axis=0, concat_axis=0, tiled=True)
    grad_y = dot2("pyzk,xpk->zyx", lines_y, x_basis)
    grad_y_sent = grad_y.astype(BF)
    modes = jnp.einsum("yzk,yj->jzk", data, basis32, precision=HIGH)
    modes = modes.reshape(pieces, kyblock, zshare, xblock)
    modes = lax.all_to_all(modes, ("band", "py"), split_axis=0, concat_axis=0, tiled=True)
    source = np.arange(points)
    device, within = source // zshare, source % zshare
    z_order = device % rows_py * zblock + device // rows_py * zshare + within
    z_basis = basis32[z_order].reshape(pieces, zshare, points)
    z_derive = derive[z_order][:, z_order].reshape(pieces, zshare, pieces, zshare)
    spectrum = jnp.einsum("djzk,dzm->mjk", modes, z_basis, precision=HIGH)
    unit = 2.0 * math.pi / (points * SPACING)
    all_q = jnp.asarray((freq * freq).astype(np.float32))
    q_col = lax.dynamic_slice_in_dim(all_q, (band_index * rows_py + py_index) * kyblock, kyblock)
    q_row = lax.dynamic_slice_in_dim(all_q, px_index * xblock, xblock)
    squared = unit**2 * (all_q[:, None, None] + q_col[None, :, None] + q_row[None, None, :])
    factor = jnp.where(squared > 0, 4.0 * math.pi / jnp.where(squared > 0, squared, 1.0), 0.0)
    spectrum = spectrum * factor
    back = jnp.stack(
        [
            jnp.einsum("mjk,dzm->djzk", spectrum, z_basis, precision=HIGH).astype(BF),
            jnp.einsum("ejwk,ewdz->djzk", modes, z_derive, precision=HIGH).astype(BF),
        ],
        1,
    )
    back, every_y, every_x = lax.optimization_barrier((back, grad_y_sent, every_x))
    every_y = gathered(every_y)
    back = lax.all_to_all(back, ("band", "py"), split_axis=0, concat_axis=0, tiled=True)
    y_basis = (high_basis.reshape(points, pieces, kyblock), low_basis.reshape(points, pieces, kyblock))
    lines = dot2("dfjzk,ydj->fyzk", back, y_basis)
    lines = lines.astype(BF).reshape(2, rows_px, yblock, zshare, xblock)
    lines = lax.all_to_all(lines, "px", split_axis=1, concat_axis=1, tiled=True)
    fields = dot2("fpyzk,xpk->fzyx", lines, x_basis)
    every_z = gathered(fields[1])
    potential = exchange_part(rho.transpose(1, 0, 2), fields[0], grad_x, grad_y, fields[1])
    every_potential = gathered(potential)
    gradient = jnp.stack([every_x.astype(F32), every_y.astype(F32), every_z.astype(F32)])
    return (every_potential.astype(F32), gradient)


def solution(mesh):
    return jax.shard_map(
        body,
        mesh=mesh,
        in_specs=(P("band", ("px", "py"), None), P("band"), P(None, "px"), P("py", "px", None)),
        out_specs=(P("py", "px", None), P(None, "py", "px", None)),
        check_vma=False,
    )
```
